32 devices in a mesh: groups: 2 (over x), expert: 8 (over z, y), dp: 2 (over core).
Axes of the slice: x: 2, y: 2, z: 4, core: 2. Of those that a mesh axis runs over, the one named last changes fastest.
Arguments:
- tokens: bfloat16 [128, 2880], P(('groups', 'expert', 'dp')), parts along dimension 0, may hold values from -6 to 6
- norm_gain: bfloat16 [2, 2880], replicated, may hold values from 0.25 to 1.75
- w_gate: bfloat16 [2, 2880, 23040], P(None, None, ('expert', 'dp')), may hold values from -0.109375 to 0.109375
- w_up: bfloat16 [2, 2880, 23040], P(None, None, ('expert', 'dp')), may hold values from -0.109375 to 0.109375
- w_down: bfloat16 [2, 23040, 2880], P(None, ('expert', 'dp')), may hold values from -0.109375 to 0.109375
- routes: int32 [2, 128, 4], P(None, ('groups', 'expert', 'dp')), parts along dimension 1, may hold values from 0 to 7, all different within a row; in each aligned block of 4 rows (0 to 3, 4 to 7, ..., all dimensions but the last counted through in order) at most 3 rows name the same one
- gates: float32 [2, 128, 4], P(None, ('groups', 'expert', 'dp')), parts along dimension 1, may hold values from 0.1 to 1
Outputs:
- mixed: bfloat16 [128, 2880], P(('groups', 'expert', 'dp')), parts along dimension 0
The draws below stay inside these ranges and needn't reach their ends.
There are 2 independent parts, one for each index of `groups`. The reference program is written for one: setup_inputs(seed, part) draws one part's arguments, and reference() takes and returns one part's arrays. A program takes and returns all parts, laid end to end along the dimension named above; an argument that names none is the same for every part. Nothing has to cross between parts.
Inputs may be any that keep to these rules, and one draw needn't show every extreme that they name: `routes`: each token names 4 different experts; among the 4 rows of one device (aligned blocks of a layer) no expert is named more than 3 times, and in every layer some device's block names some expert exactly 3 times.
All inputs are finite; a program needn't handle non-finite values.
Results may differ from the reference program's by a relative error of at most 0.014.
Values may be sent and summed in bfloat16 or wider, within the bound.
No kernel may reach another device: no remote copies, remote signals or barrier semaphores. Data moves between devices by JAX's collectives and lax.ppermute only.
A program may use at most 128 MiB of HBM per device.

```python
import math
import jax
import jax.numpy as jnp
import numpy as np
from jax import lax

D = 2880
FF = 2880
TOP = 4
LAYERS = 2
TOK_DEV = 4
EXPERTS = 8
CAP = 3
TOKENS = 64


def level_of(stream_key, extent, shards, smallest, top_value):
    level, own = 1.0, jax.random.fold_in(stream_key, 6)
    for position, parts in shards:
        heights = jnp.exp(jax.random.uniform(jax.random.fold_in(own, position), (parts,), jnp.float32, smallest / len(shards), top_value / len(shards)))
        level = level * jnp.repeat(heights, extent[position] // parts).reshape([-1 if axis == position else 1 for axis in range(len(extent))])
    return level


def shared_out(own_key, own, number, rows, amount, top, most, slope):
    ranking = jax.random.permutation(own_key, amount)
    crowded, common = shares(amount, rows * top, most, slope, True), shares(amount, rows * top, most, slope, False)
    places = jnp.arange(amount)

    def named(tallies, rotation):
        used = int((tallies > 0).sum())
        fixed = max(1, used // 4)
        shifted = fixed + (places - fixed + rotation * (used - fixed)) % max(1, amount - fixed)
        return jnp.zeros((amount,), jnp.int32).at[ranking[jnp.where(places < fixed, places, shifted)]].set(jnp.asarray(tallies, jnp.int32))

    tallies = jnp.where(number % 4 == 0, named(crowded, number // 4), named(common, number - number // 4 - 1))
    mixed = jax.random.permutation(jax.random.fold_in(own, 3), amount)
    source_of, receiver = mixed[0:amount // 2 * 2:2], mixed[1:amount // 2 * 2:2]
    room = jnp.minimum(tallies[source_of] - 1, most - tallies[receiver]) // 2
    room = jnp.where((source_of == ranking[0]) | (receiver == ranking[0]) | (tallies[receiver] == 0), 0, jnp.maximum(room, 0))
    shifted = jax.random.randint(jax.random.fold_in(own, 4), (amount // 2,), 0, 1 << 20) % (room + 1)
    tallies = tallies.at[source_of].add(-shifted).at[receiver].add(shifted)
    labels = jnp.searchsorted(jnp.cumsum(tallies), jnp.arange(rows * top), side="right").astype(jnp.int32)
    listing = labels.reshape(top, rows).T
    listing = listing[jax.random.permutation(jax.random.fold_in(own, 1), rows)]
    rotation = jax.random.randint(jax.random.fold_in(own, 2), (rows, 1), 0, top)
    return jnp.take_along_axis(listing, (jnp.arange(top)[None, :] + rotation) % top, axis=1)


def shares(amount, total, bound, lean, full):
    weights = [(1 << 20) // math.isqrt(standing ** lean) + 1 for standing in range(1, amount + 1)]
    largest = bound if full else min(bound, max(-(-total // amount), total * weights[0] // sum(weights)))
    least = 1 if total - largest >= amount - 1 else 0
    given, rest = [largest] + [least] * (amount - 1), total - largest - least * (amount - 1)
    while rest > 0:
        movable = [i for i in range(1, amount) if given[i] < largest] or [i for i in range(1, amount) if given[i] < bound]
        pool, left = sum([weights[i] for i in movable]), rest
        for i in movable:
            more = min(bound - given[i], max(1, left * weights[i] // pool), rest)
            given[i] = given[i] + more
            rest = rest - more
    return np.array(given)


def normal_values(own_key, extent, width, bound, shards=(), kind=jnp.bfloat16):
    drawn = jax.random.normal(own_key, extent, jnp.float32) * width
    if len(shards) > 0:
        drawn = level_of(own_key, extent, shards, -0.22, 0.18) * drawn
    return jnp.clip(drawn, min=-bound, max=bound).astype(kind)


def setup_inputs(seed: int = 0, part: int = 0) -> dict:
    key_of = jax.random.split(jax.random.key(seed), 8)
    part_splits = jax.random.split(jax.random.fold_in(key_of[7], part), 8)
    tokens = normal_values(part_splits[0], (TOKENS, D), 1.0, 6.0, ((0, 16),))
    norm_gain = jnp.clip(1.0 + 0.15 * jax.random.normal(key_of[1], (LAYERS, D), jnp.float32), 0.25, 1.75).astype(jnp.bfloat16)
    w_gate = normal_values(key_of[2], (LAYERS, D, EXPERTS * FF), D ** -0.5, 0.109375, ((2, 16),))
    w_up = normal_values(key_of[3], (LAYERS, D, EXPERTS * FF), D ** -0.5, 0.109375, ((2, 16),))
    w_down = normal_values(key_of[4], (LAYERS, EXPERTS * FF, D), FF ** -0.5, 0.109375, ((1, 16),))
    routes_keys = jax.random.split(jax.random.fold_in(part_splits[5], 1), LAYERS * TOKENS // TOK_DEV)
    routes_turns = jax.random.permutation(jax.random.fold_in(part_splits[5], 3), LAYERS * TOKENS // TOK_DEV)
    routes = jax.vmap(lambda own, number: shared_out(jax.random.fold_in(part_splits[5], 2), own, number, TOK_DEV, EXPERTS, TOP, CAP, 2))(routes_keys, routes_turns).reshape((LAYERS, TOKENS, TOP))
    gates = jnp.clip(0.1 + 0.9 * jax.random.uniform(part_splits[6], (LAYERS, TOKENS, TOP), jnp.float32) ** level_of(part_splits[6], (LAYERS, TOKENS, TOP), ((1, 16),), -0.2, 0.2), 0.1, 1.0)
    return dict(tokens=tokens, norm_gain=norm_gain, w_gate=w_gate, w_up=w_up, w_down=w_down, routes=routes, gates=gates)


def rms_normed(hidden_state, gain_row):
    widened = hidden_state.astype(jnp.float32)
    scale_inv = lax.rsqrt(lax.optimization_barrier(jnp.mean(widened * widened, axis=-1, keepdims=True)) + 1e-05)
    return (widened * scale_inv * gain_row.astype(jnp.float32)).astype(jnp.bfloat16)

def reference(tokens, norm_gain, w_gate, w_up, w_down, routes, gates):
    block_count = TOKENS // TOK_DEV
    hidden_state = tokens
    for layer_idx in range(LAYERS):
        widened = hidden_state.astype(jnp.float32)
        normed = rms_normed(hidden_state, norm_gain[layer_idx])
        expert_ids = routes[layer_idx].reshape(block_count, TOK_DEV * TOP)
        one_hot = (expert_ids[:, :, None] == jnp.arange(EXPERTS, dtype=jnp.int32)[None, None, :]).astype(jnp.int32)
        slot_index = lax.optimization_barrier(jnp.sum((jnp.cumsum(one_hot, axis=1) - one_hot) * one_hot, axis=2))
        block_ids = jnp.arange(block_count, dtype=jnp.int32)[:, None]
        row_index = (expert_ids * (block_count * CAP) + block_ids * CAP + slot_index).reshape(-1).astype(jnp.int32)
        token_index = jnp.arange(TOKENS * TOP, dtype=jnp.int32) // TOP
        packed = jnp.zeros((EXPERTS * block_count * CAP, D), jnp.bfloat16).at[row_index].set(normed[token_index])
        packed = packed.reshape(EXPERTS, block_count * CAP, D)
        gate_layer = w_gate[layer_idx]
        up_layer = w_up[layer_idx]
        down_layer = w_down[layer_idx]

        def one_expert(expert_num):
            col_start = (expert_num * FF).astype(jnp.int32)
            inputs_f = lax.dynamic_index_in_dim(packed, expert_num, 0, keepdims=False).astype(jnp.float32)
            gate_cols = lax.dynamic_slice_in_dim(gate_layer, col_start, FF, 1).astype(jnp.float32)
            up_cols = lax.dynamic_slice_in_dim(up_layer, col_start, FF, 1).astype(jnp.float32)
            down_rows = lax.dynamic_slice_in_dim(down_layer, col_start, FF, 0).astype(jnp.float32)
            gate_val = jnp.dot(inputs_f, gate_cols)
            up_val = jnp.dot(inputs_f, up_cols)
            active = (gate_val * jax.nn.sigmoid(1.702 * gate_val) * (up_val + 1.0)).astype(jnp.bfloat16)
            active = lax.optimization_barrier(active).astype(jnp.float32)
            return jnp.dot(active, down_rows)
        expert_out = lax.map(one_expert, jnp.arange(EXPERTS, dtype=jnp.int32))
        route_out = expert_out.reshape(-1, D)[row_index].reshape(TOKENS, TOP, D)
        mixture = lax.optimization_barrier(jnp.sum(route_out * gates[layer_idx][:, :, None].astype(jnp.float32), axis=1))
        hidden_state = (widened + mixture).astype(jnp.bfloat16)
    return hidden_state
```

```python
import functools

import jax
import jax.numpy as jnp
from jax import lax
from jax.experimental import pallas as pl
from jax.experimental.pallas import tpu as pltpu
from jax.sharding import PartitionSpec as P

EPS = 1e-05
VMEM_LIMIT = 20 * 1024 * 1024


def normalise(value, gain_row):
    scale_inv = lax.rsqrt(jnp.mean(value * value, axis=-1, keepdims=True) + EPS)
    return (value * scale_inv * gain_row.astype(jnp.float32)).astype(jnp.bfloat16)


def first_norm_kernel(tokens_ref, gain_ref, normed_ref):
    normed_ref[...] = normalise(tokens_ref[...].astype(jnp.float32), gain_ref[0:1, :])


def first_norm(tokens, norm_gain):
    return pl.pallas_call(
        first_norm_kernel,
        out_shape=jax.ShapeDtypeStruct(tokens.shape, jnp.bfloat16),
        name="first_norm",
    )(tokens, norm_gain)


def hidden_block(hidden):
    for block in (240, 480, 288, 144, 96, 720):
        if hidden % block == 0:
            return block
    return hidden


def experts_kernel(mine_ref, other_ref, gate_ref, up_ref, down_ref, keep_ref, send_ref, rows_ref, acc_ref):
    step = pl.program_id(0)
    half = mine_ref.shape[0]

    @pl.when(step == 0)
    def _():
        rows_ref[:half, :] = mine_ref[...]
        rows_ref[half:, :] = other_ref[...]

    rows = rows_ref[...]
    across = (((1,), (1,)), ((), ()))
    gate_val = lax.dot_general(rows, gate_ref[0], across, preferred_element_type=jnp.float32)
    up_val = lax.dot_general(rows, up_ref[0], across, preferred_element_type=jnp.float32)
    active = (gate_val * jax.nn.sigmoid(1.702 * gate_val) * (up_val + 1.0)).astype(jnp.bfloat16)
    part = jnp.dot(active, down_ref[0], preferred_element_type=jnp.float32)

    @pl.when(step == 0)
    def _():
        acc_ref[...] = part

    @pl.when(step > 0)
    def _():
        acc_ref[...] += part

    @pl.when(step == pl.num_programs(0) - 1)
    def _():
        keep_ref[...] = acc_ref[:half, :].astype(jnp.bfloat16)
        send_ref[...] = acc_ref[half:, :].astype(jnp.bfloat16)


def experts(layer_idx, mine, other, gate_rows, up_rows, down_rows):
    half, width = mine.shape
    hidden = down_rows.shape[1]
    block = hidden_block(hidden)
    whole = pl.BlockSpec((half, width), lambda i: (0, 0))
    weight = pl.BlockSpec((1, block, width), lambda i: (layer_idx, i, 0))
    return pl.pallas_call(
        experts_kernel,
        grid=(hidden // block,),
        in_specs=[whole, whole, weight, weight, weight],
        out_specs=[whole, whole],
        out_shape=[jax.ShapeDtypeStruct((half, width), jnp.bfloat16)] * 2,
        scratch_shapes=[
            pltpu.VMEM((2 * half, width), jnp.bfloat16),
            pltpu.VMEM((2 * half, width), jnp.float32),
        ],
        compiler_params=pltpu.CompilerParams(vmem_limit_bytes=VMEM_LIMIT),
        name="experts",
    )(mine, other, gate_rows, up_rows, down_rows)


def combine_kernel(layer_idx, chips_per_expert, last, state_ref, parts_ref, routes_ref, gates_ref, gain_ref, *out_refs):
    routes = routes_ref[layer_idx]
    gates = gates_ref[layer_idx]
    total = jnp.zeros(state_ref.shape, jnp.float32)
    for chip in range(parts_ref.shape[0]):
        weight = jnp.sum(jnp.where(routes == chip // chips_per_expert, gates, 0.0), axis=1, keepdims=True)
        total = total + weight * parts_ref[chip].astype(jnp.float32)
    state = (state_ref[...].astype(jnp.float32) + total).astype(jnp.bfloat16)
    out_refs[0][...] = state
    if not last:
        out_refs[1][...] = normalise(state.astype(jnp.float32), gain_ref[layer_idx + 1 : layer_idx + 2, :])


def combine(layer_idx, last, chips_per_expert, state, parts, routes, gates, norm_gain):
    shape = jax.ShapeDtypeStruct(state.shape, jnp.bfloat16)
    return pl.pallas_call(
        functools.partial(combine_kernel, layer_idx, chips_per_expert, last),
        out_shape=[shape] if last else [shape, shape],
        compiler_params=pltpu.CompilerParams(vmem_limit_bytes=VMEM_LIMIT),
        name="combine",
    )(state, parts, routes, gates, norm_gain)


def on_device(tokens, norm_gain, w_gate, w_up, w_down, routes, gates):
    token_count, width = tokens.shape
    layers = norm_gain.shape[0]
    chips = lax.axis_size("expert")
    pair_size = lax.axis_size("dp")
    expert_total = chips * pair_size * w_down.shape[1] // width
    chips_per_expert = chips // expert_total
    swap = [(0, 1), (1, 0)]
    gate_rows = jnp.swapaxes(w_gate, 1, 2)
    up_rows = jnp.swapaxes(w_up, 1, 2)
    state = tokens
    normed = first_norm(tokens, norm_gain)
    for layer_idx in range(layers):
        outgoing = jnp.broadcast_to(normed[None], (chips, token_count, width))
        arrived = lax.all_to_all(outgoing, "expert", split_axis=0, concat_axis=0, tiled=True)
        mine = arrived.reshape(chips * token_count, width)
        other = lax.ppermute(mine, "dp", swap)
        keep, send = experts(layer_idx, mine, other, gate_rows, up_rows, w_down)
        got = lax.ppermute(send, "dp", swap)
        paired = (keep + got).reshape(chips, token_count, width)
        parts = lax.all_to_all(paired, "expert", split_axis=0, concat_axis=0, tiled=True)
        last = layer_idx == layers - 1
        results = combine(layer_idx, last, chips_per_expert, state, parts, routes, gates, norm_gain)
        state = results[0]
        normed = results[-1]
    return state


def solution(mesh):
    return jax.shard_map(
        on_device,
        mesh=mesh,
        in_specs=(
            P(("groups", "expert", "dp"), None),
            P(),
            P(None, None, ("expert", "dp")),
            P(None, None, ("expert", "dp")),
            P(None, ("expert", "dp"), None),
            P(None, ("groups", "expert", "dp"), None),
            P(None, ("groups", "expert", "dp"), None),
        ),
        out_specs=P(("groups", "expert", "dp"), None),
        check_vma=False,
    )
```

```python
import functools

import jax
import jax.numpy as jnp
from jax import lax
from jax.experimental import pallas as pl
from jax.experimental.pallas import tpu as pltpu
from jax.sharding import PartitionSpec as P

EPS = 1e-05
VMEM_LIMIT = 50 * 1024 * 1024


def normalise(value, gain_row):
    scale_inv = lax.rsqrt(jnp.mean(value * value, axis=-1, keepdims=True) + EPS)
    return (value * scale_inv * gain_row.astype(jnp.float32)).astype(jnp.bfloat16)


def first_norm_kernel(tokens_ref, gain_ref, normed_ref):
    normed_ref[...] = normalise(tokens_ref[...].astype(jnp.float32), gain_ref[0:1, :])


def first_norm(tokens, norm_gain):
    return pl.pallas_call(
        first_norm_kernel,
        out_shape=jax.ShapeDtypeStruct(tokens.shape, jnp.bfloat16),
        name="first_norm",
    )(tokens, norm_gain)


def hidden_block(hidden):
    for block in (240, 480, 288, 144, 96, 720):
        if hidden % block == 0:
            return block
    return hidden


def experts_kernel(mine_ref, other_ref, gate_ref, up_ref, down_ref, keep_ref, send_ref, rows_ref, acc_ref):
    step = pl.program_id(0)
    half = mine_ref.shape[0]

    @pl.when(step == 0)
    def _():
        rows_ref[:half, :] = mine_ref[...]
        rows_ref[half:, :] = other_ref[...]

    rows = rows_ref[...]
    across = (((1,), (1,)), ((), ()))
    gate_val = lax.dot_general(rows, gate_ref[0], across, preferred_element_type=jnp.float32)
    up_val = lax.dot_general(rows, up_ref[0], across, preferred_element_type=jnp.float32)
    active = (gate_val * jax.nn.sigmoid(1.702 * gate_val) * (up_val + 1.0)).astype(jnp.bfloat16)
    part = jnp.dot(active, down_ref[0], preferred_element_type=jnp.float32)

    @pl.when(step == 0)
    def _():
        acc_ref[...] = part

    @pl.when(step > 0)
    def _():
        acc_ref[...] += part

    @pl.when(step == pl.num_programs(0) - 1)
    def _():
        keep_ref[...] = acc_ref[:half, :].astype(jnp.bfloat16)
        send_ref[...] = acc_ref[half:, :].astype(jnp.bfloat16)


def experts(layer_idx, mine, other, gate_rows, up_rows, down_rows):
    half, width = mine.shape
    hidden = down_rows.shape[1]
    block = hidden_block(hidden)
    whole = pl.BlockSpec(memory_space=pltpu.VMEM)
    weight = pl.BlockSpec((1, block, width), lambda i: (layer_idx, i, 0))
    return pl.pallas_call(
        experts_kernel,
        grid=(hidden // block,),
        in_specs=[whole, whole, weight, weight, weight],
        out_specs=[whole, whole],
        out_shape=[jax.ShapeDtypeStruct((half, width), jnp.bfloat16)] * 2,
        scratch_shapes=[
            pltpu.VMEM((2 * half, width), jnp.bfloat16),
            pltpu.VMEM((2 * half, width), jnp.float32),
        ],
        compiler_params=pltpu.CompilerParams(vmem_limit_bytes=VMEM_LIMIT),
        name="experts",
    )(mine, other, gate_rows, up_rows, down_rows)


def combine_kernel(layer_idx, chips_per_expert, last, state_ref, parts_ref, routes_ref, gates_ref, gain_ref, *out_refs):
    routes = routes_ref[layer_idx]
    gates = gates_ref[layer_idx]
    total = jnp.zeros(state_ref.shape, jnp.float32)
    for chip in range(parts_ref.shape[0]):
        weight = jnp.sum(jnp.where(routes == chip // chips_per_expert, gates, 0.0), axis=1, keepdims=True)
        total = total + weight * parts_ref[chip].astype(jnp.float32)
    state = (state_ref[...].astype(jnp.float32) + total).astype(jnp.bfloat16)
    out_refs[0][...] = state
    if not last:
        out_refs[1][...] = normalise(state.astype(jnp.float32), gain_ref[layer_idx + 1 : layer_idx + 2, :])


def combine(layer_idx, last, chips_per_expert, state, parts, routes, gates, norm_gain):
    shape = jax.ShapeDtypeStruct(state.shape, jnp.bfloat16)
    return pl.pallas_call(
        functools.partial(combine_kernel, layer_idx, chips_per_expert, last),
        out_shape=[shape] if last else [shape, shape],
        name="combine",
    )(state, parts, routes, gates, norm_gain)


def on_device(tokens, norm_gain, w_gate, w_up, w_down, routes, gates):
    token_count, width = tokens.shape
    layers = norm_gain.shape[0]
    chips = lax.axis_size("expert")
    pair_size = lax.axis_size("dp")
    expert_total = chips * pair_size * w_down.shape[1] // width
    chips_per_expert = chips // expert_total
    swap = [(0, 1), (1, 0)]
    gate_rows = jnp.swapaxes(w_gate, 1, 2)
    up_rows = jnp.swapaxes(w_up, 1, 2)
    state = tokens
    normed = first_norm(tokens, norm_gain)
    for layer_idx in range(layers):
        outgoing = jnp.broadcast_to(normed[None], (chips, token_count, width))
        arrived = lax.all_to_all(outgoing, "expert", split_axis=0, concat_axis=0, tiled=True)
        mine = arrived.reshape(chips * token_count, width)
        other = lax.ppermute(mine, "dp", swap)
        keep, send = experts(layer_idx, mine, other, gate_rows, up_rows, w_down)
        got = lax.ppermute(send, "dp", swap)
        paired = (keep + got).reshape(chips, token_count, width)
        parts = lax.all_to_all(paired, "expert", split_axis=0, concat_axis=0, tiled=True)
        last = layer_idx == layers - 1
        results = combine(layer_idx, last, chips_per_expert, state, parts, routes, gates, norm_gain)
        state = results[0]
        normed = results[-1]
    return state


def solution(mesh):
    return jax.shard_map(
        on_device,
        mesh=mesh,
        in_specs=(
            P(("groups", "expert", "dp"), None),
            P(),
            P(None, None, ("expert", "dp")),
            P(None, None, ("expert", "dp")),
            P(None, ("expert", "dp"), None),
            P(None, ("groups", "expert", "dp"), None),
            P(None, ("groups", "expert", "dp"), None),
        ),
        out_specs=P(("groups", "expert", "dp"), None),
        check_vma=False,
    )
```

```python
import functools

import jax
import jax.numpy as jnp
from jax import lax
from jax.experimental import pallas as pl
from jax.experimental.pallas import tpu as pltpu
from jax.sharding import PartitionSpec as P

EPS = 1e-05
VMEM_LIMIT = 50 * 1024 * 1024


def normalise(value, gain_row):
    scale_inv = lax.rsqrt(jnp.mean(value * value, axis=-1, keepdims=True) + EPS)
    return (value * scale_inv * gain_row.astype(jnp.float32)).astype(jnp.bfloat16)


def first_norm_kernel(tokens_ref, gain_ref, normed_ref):
    normed_ref[...] = normalise(tokens_ref[...].astype(jnp.float32), gain_ref[0:1, :])


def first_norm(tokens, norm_gain):
    return pl.pallas_call(
        first_norm_kernel,
        in_specs=[pl.BlockSpec(memory_space=pltpu.VMEM)] * 2,
        out_specs=pl.BlockSpec(memory_space=pltpu.VMEM),
        out_shape=jax.ShapeDtypeStruct(tokens.shape, jnp.bfloat16),
        name="first_norm",
    )(tokens, norm_gain)


def hidden_block(hidden):
    for block in (480, 240, 288, 144, 96):
        if hidden % block == 0:
            return block
    return hidden


def experts_kernel(mine_ref, other_ref, gate_ref, up_ref, down_ref, keep_ref, send_ref, rows_ref, acc_ref):
    step = pl.program_id(0)
    half = mine_ref.shape[0]

    @pl.when(step == 0)
    def _():
        rows_ref[:half, :] = mine_ref[...]
        rows_ref[half:, :] = other_ref[...]

    rows = rows_ref[...]
    across = (((1,), (1,)), ((), ()))
    gate_val = lax.dot_general(rows, gate_ref[0], across, preferred_element_type=jnp.float32)
    up_val = lax.dot_general(rows, up_ref[0], across, preferred_element_type=jnp.float32)
    active = (gate_val * jax.nn.sigmoid(1.702 * gate_val) * (up_val + 1.0)).astype(jnp.bfloat16)
    part = jnp.dot(active, down_ref[0], preferred_element_type=jnp.float32)

    @pl.when(step == 0)
    def _():
        acc_ref[...] = part

    @pl.when(step > 0)
    def _():
        acc_ref[...] += part

    @pl.when(step == pl.num_programs(0) - 1)
    def _():
        keep_ref[...] = acc_ref[:half, :].astype(jnp.bfloat16)
        send_ref[...] = acc_ref[half:, :].astype(jnp.bfloat16)


def experts(layer_idx, mine, other, gate_rows, up_rows, down_rows):
    half, width = mine.shape
    hidden = down_rows.shape[1]
    block = hidden_block(hidden)
    whole = pl.BlockSpec(memory_space=pltpu.VMEM)
    weight = pl.BlockSpec((1, block, width), lambda i: (layer_idx, i, 0))
    return pl.pallas_call(
        experts_kernel,
        grid=(hidden // block,),
        in_specs=[whole, whole, weight, weight, weight],
        out_specs=[whole, whole],
        out_shape=[jax.ShapeDtypeStruct((half, width), jnp.bfloat16)] * 2,
        scratch_shapes=[
            pltpu.VMEM((2 * half, width), jnp.bfloat16),
            pltpu.VMEM((2 * half, width), jnp.float32),
        ],
        compiler_params=pltpu.CompilerParams(vmem_limit_bytes=VMEM_LIMIT),
        name="experts",
    )(mine, other, gate_rows, up_rows, down_rows)


def combine_kernel(layer_idx, chips_per_expert, last, state_ref, parts_ref, routes_ref, gates_ref, gain_ref, *out_refs):
    routes = routes_ref[layer_idx]
    gates = gates_ref[layer_idx]
    total = jnp.zeros(state_ref.shape, jnp.float32)
    for chip in range(parts_ref.shape[0]):
        weight = jnp.sum(jnp.where(routes == chip // chips_per_expert, gates, 0.0), axis=1, keepdims=True)
        total = total + weight * parts_ref[chip].astype(jnp.float32)
    state = (state_ref[...].astype(jnp.float32) + total).astype(jnp.bfloat16)
    out_refs[0][...] = state
    if not last:
        out_refs[1][...] = normalise(state.astype(jnp.float32), gain_ref[layer_idx + 1 : layer_idx + 2, :])


def combine(layer_idx, last, chips_per_expert, state, parts, routes, gates, norm_gain):
    shape = jax.ShapeDtypeStruct(state.shape, jnp.bfloat16)
    whole = pl.BlockSpec(memory_space=pltpu.VMEM)
    return pl.pallas_call(
        functools.partial(combine_kernel, layer_idx, chips_per_expert, last),
        in_specs=[whole] * 5,
        out_specs=[whole] if last else [whole, whole],
        out_shape=[shape] if last else [shape, shape],
        name="combine",
    )(state, parts, routes, gates, norm_gain)


def on_device(tokens, norm_gain, w_gate, w_up, w_down, routes, gates):
    token_count, width = tokens.shape
    layers = norm_gain.shape[0]
    chips = lax.axis_size("expert")
    pair_size = lax.axis_size("dp")
    expert_total = chips * pair_size * w_down.shape[1] // width
    chips_per_expert = chips // expert_total
    swap = [(0, 1), (1, 0)]
    gate_rows = jnp.swapaxes(w_gate, 1, 2)
    up_rows = jnp.swapaxes(w_up, 1, 2)
    state = tokens
    normed = first_norm(tokens, norm_gain)
    for layer_idx in range(layers):
        outgoing = jnp.broadcast_to(normed[None], (chips, token_count, width))
        arrived = lax.all_to_all(outgoing, "expert", split_axis=0, concat_axis=0, tiled=True)
        mine = arrived.reshape(chips * token_count, width)
        other = lax.ppermute(mine, "dp", swap)
        keep, send = experts(layer_idx, mine, other, gate_rows, up_rows, w_down)
        got = lax.ppermute(send, "dp", swap)
        paired = (keep + got).reshape(chips, token_count, width)
        parts = lax.all_to_all(paired, "expert", split_axis=0, concat_axis=0, tiled=True)
        last = layer_idx == layers - 1
        results = combine(layer_idx, last, chips_per_expert, state, parts, routes, gates, norm_gain)
        state = results[0]
        normed = results[-1]
    return state


def solution(mesh):
    return jax.shard_map(
        on_device,
        mesh=mesh,
        in_specs=(
            P(("groups", "expert", "dp"), None),
            P(),
            P(None, None, ("expert", "dp")),
            P(None, None, ("expert", "dp")),
            P(None, ("expert", "dp"), None),
            P(None, ("groups", "expert", "dp"), None),
            P(None, ("groups", "expert", "dp"), None),
        ),
        out_specs=P(("groups", "expert", "dp"), None),
        check_vma=False,
    )
```
